32 devices in a mesh: dp: 32 (over z, y, x, core).
Axes of the slice: x: 2, y: 2, z: 4, core: 2. Of those that a mesh axis runs over, the one named last changes fastest.
Arguments:
- block_input: bfloat16 [8192, 3072], P('dp'), may hold values from -12 to 12
- segments: int32 [8192], P('dp'), may hold values from 0 to 8191, as said below
- cotangent: bfloat16 [8192, 3072], P('dp'), may hold values from -6 to 6
- gain_one: bfloat16 [3072], P('dp'), may hold values from 0.5 to 1.5
- w_z: bfloat16 [3072, 3072], P('dp'), may hold values from -0.109375 to 0.109375
- w_x: bfloat16 [3072, 3072], P('dp'), may hold values from -0.109375 to 0.109375
- w_bc: bfloat16 [3072, 512], P('dp'), may hold values from -0.109375 to 0.109375
- w_dt: bfloat16 [3072, 24], P('dp'), may hold values from -0.109375 to 0.109375
- conv_weight: bfloat16 [4, 3584], P(None, 'dp'), may hold values from -0.59765625 to 0.59765625
- conv_bias: bfloat16 [3584], P('dp'), may hold values from -3 to 3
- head_params: float32 [3, 24], replicated, may hold values from -3 to 1
- w_mout: bfloat16 [3072, 3072], P('dp'), may hold values from -0.109375 to 0.109375
- w_q: bfloat16 [3072, 1536], P('dp'), may hold values from -1 to 1
- w_kv: bfloat16 [3072, 512], P('dp'), may hold values from -1 to 1
- w_ao: bfloat16 [1536, 3072], P('dp'), may hold values from -0.4375 to 0.4375
- gain_two: bfloat16 [3072], P('dp'), may hold values from 0.5 to 1.5
- w_gate: bfloat16 [3072, 12288], P('dp'), may hold values from -0.109375 to 0.109375
- w_up: bfloat16 [3072, 12288], P('dp'), may hold values from -0.109375 to 0.109375
- w_down: bfloat16 [12288, 3072], P('dp'), may hold values from -0.0546875 to 0.0546875
Outputs:
- block_out: bfloat16 [8192, 3072], P('dp')
- grad_input: bfloat16 [8192, 3072], P('dp')
- grad_gain_one: float32 [3072], P('dp')
- grad_w_z: float32 [3072, 3072], P('dp')
- grad_w_x: float32 [3072, 3072], P('dp')
- grad_w_bc: float32 [3072, 512], P('dp')
- grad_w_dt: float32 [3072, 24], P('dp')
- grad_conv_weight: float32 [4, 3584], P(None, 'dp')
- grad_conv_bias: float32 [3584], P('dp')
- grad_head_params: float32 [3, 24], replicated
- grad_w_mout: float32 [3072, 3072], P('dp')
- grad_w_q: float32 [3072, 1536], P('dp')
- grad_w_kv: float32 [3072, 512], P('dp')
- grad_w_ao: float32 [1536, 3072], P('dp')
- grad_gain_two: float32 [3072], P('dp')
- grad_w_gate: float32 [3072, 12288], P('dp')
- grad_w_up: float32 [3072, 12288], P('dp')
- grad_w_down: float32 [12288, 3072], P('dp')
The draws below stay inside these ranges and needn't reach their ends.
Inputs may be any that keep to these rules, and one draw needn't show every extreme that they name: `segments`: each token holds the global index of the first token of its sequence; a sequence lies within one aligned block of 256 tokens; in every draw some block is one sequence of 256 tokens, and the last token is a sequence of its own.
All inputs are finite; a program needn't handle non-finite values.
Results may differ from the reference program's by a relative error of at most 0.012.
Values may be sent and summed in bfloat16 or wider, within the bound.
A program may use at most 1.125 GiB of HBM per device.

```python
import jax
import jax.numpy as jnp
from jax import lax

D = 3072
FF = 12288
HEADS = 24
HDIM = 128
NSTATE = 256
KCONV = 4
QHEADS = 12
KVHEADS = 2
ROWS = 256
TOKENS = 8192
DSSM = 3072
CONVCH = 3584
QW = 1536


def draw_segments(key, part):
    blocks = TOKENS // ROWS
    first_key, second_key = jax.random.split(key)
    starts = jax.random.randint(first_key, (blocks, ROWS), 0, 40) == 0
    starts = starts.at[:, 0].set(True)
    starts = starts.at[blocks - 1, ROWS - 1].set(True)
    chosen = jax.random.randint(second_key, (), 0, blocks - 1)
    whole = (jnp.arange(blocks) == chosen)[:, None] & (jnp.arange(ROWS)[None, :] > 0)
    starts = starts & jnp.logical_not(whole)
    index = jnp.arange(TOKENS, dtype=jnp.int32).reshape(blocks, ROWS)
    marked = jnp.where(starts, index, 0)
    return lax.cummax(marked, axis=1).reshape(TOKENS).astype(jnp.int32)


def draw_block_input(key, part):
    rough = jax.random.truncated_normal(jax.random.fold_in(key, 201), -6.0, 6.0, (TOKENS, D), jnp.float32)
    values = rough
    return values.astype(jnp.bfloat16)


def key_basis(key):
    raw = jax.random.truncated_normal(jax.random.fold_in(key, 101), -6.0, 6.0, (D, KVHEADS * HDIM), jnp.float32)
    return raw * D ** (-0.5)


def draw_w_kv(key, part):
    keys_part = key_basis(key)
    values_part = jax.random.truncated_normal(jax.random.fold_in(key, 102), -6.0, 6.0, (D, KVHEADS * HDIM), jnp.float32) * D ** (-0.5)
    return jnp.concatenate([keys_part, values_part], axis=1).astype(jnp.bfloat16)


def draw_w_q(key, part):
    own = jax.random.truncated_normal(jax.random.fold_in(key, 103), -6.0, 6.0, (D, QHEADS * HDIM), jnp.float32) * D ** (-0.5)
    values = own
    return values.astype(jnp.bfloat16)


def steps_of(key, extent, shards, smallest, top_value):
    level = 1.0
    for dim, blocks in shards:
        heights = jax.random.uniform(jax.random.fold_in(jax.random.fold_in(key, 6), dim), (blocks,), jnp.float32, smallest / len(shards), top_value / len(shards))
        level = level * jnp.repeat(jnp.exp(heights), extent[dim] // blocks).reshape((-1,) + (1,) * (len(extent) - 1 - dim))
    return level


def bell_draw(key, extent, scale, limit, cuts=(), kind=jnp.bfloat16):
    entries = scale * jax.random.normal(key, extent, jnp.float32)
    if cuts:
        entries = entries * steps_of(key, extent, cuts, -0.22, 0.18)
    return jnp.clip(entries, -limit, limit).astype(kind)


def setup_inputs(seed: int = 0) -> dict:
    arg_keys = jax.random.split(jax.random.key(seed), 20)
    return {
        "block_input": draw_block_input(jax.random.fold_in(arg_keys[19], 71), 0),
        "segments": draw_segments(jax.random.fold_in(arg_keys[19], 71), 0),
        "cotangent": bell_draw(arg_keys[2], (TOKENS, D), 1.0, 6.0, ((0, 32),)),
        "gain_one": jnp.clip(1.0 + 0.1 * jax.random.normal(arg_keys[3], (D,), jnp.float32), 0.5, 1.5).astype(jnp.bfloat16),
        "w_z": bell_draw(arg_keys[4], (D, DSSM), D ** -0.5, 0.109375, ((0, 32),)),
        "w_x": bell_draw(arg_keys[5], (D, DSSM), D ** -0.5, 0.109375, ((0, 32),)),
        "w_bc": bell_draw(arg_keys[6], (D, 2 * NSTATE), D ** -0.5, 0.109375, ((0, 32),)),
        "w_dt": bell_draw(arg_keys[7], (D, HEADS), D ** -0.5, 0.109375, ((0, 32),)),
        "conv_weight": jnp.clip(jax.random.uniform(arg_keys[8], (KCONV, CONVCH), jnp.float32, -0.59765625, 0.59765625) * steps_of(arg_keys[8], (KCONV, CONVCH), ((1, 32),), -0.4, 0.0), -0.59765625, 0.59765625).astype(jnp.bfloat16),
        "conv_bias": bell_draw(arg_keys[9], (CONVCH,), 0.5, 3.0, ((0, 32),)),
        "head_params": jnp.clip(jax.random.uniform(arg_keys[10], (3, HEADS), jnp.float32, -3.0, 1.0), -3.0, 1.0),
        "w_mout": bell_draw(arg_keys[11], (DSSM, D), DSSM ** -0.5, 0.109375, ((0, 32),)),
        "w_q": draw_w_q(jax.random.fold_in(arg_keys[19], 71), 0),
        "w_kv": draw_w_kv(jax.random.fold_in(arg_keys[19], 71), 0),
        "w_ao": bell_draw(arg_keys[14], (QW, D), (QW // 8) ** -0.5, 0.4375, ((0, 32),)),
        "gain_two": jnp.clip(1.0 + 0.1 * jax.random.normal(arg_keys[15], (D,), jnp.float32), 0.5, 1.5).astype(jnp.bfloat16),
        "w_gate": bell_draw(arg_keys[16], (D, FF), D ** -0.5, 0.109375, ((0, 32),)),
        "w_up": bell_draw(arg_keys[17], (D, FF), D ** -0.5, 0.109375, ((0, 32),)),
        "w_down": bell_draw(arg_keys[18], (FF, D), FF ** -0.5, 0.0546875, ((0, 32),)),
    }


EPS = 1e-05
ROPE_BASE = 100000000000.0

def matmul(left, right):
    return jnp.dot(left, right, preferred_element_type=jnp.float32)

def mat_bt(left, right):
    return lax.dot_general(left, right, (((1,), (1,)), ((), ())), preferred_element_type=jnp.float32)

def mat_at(left, right):
    return lax.dot_general(left, right, (((0,), (0,)), ((), ())), preferred_element_type=jnp.float32)

def norm_forward(values, gain):
    rstd = lax.rsqrt(lax.optimization_barrier(jnp.mean(values * values, axis=-1, keepdims=True)) + EPS)
    normed = values * rstd
    return (normed, rstd, (normed * gain.astype(jnp.float32)).astype(jnp.bfloat16))

def norm_backward(grad_out, normed, rstd, gain):
    scaled = grad_out * gain.astype(jnp.float32)
    grad_in = rstd * (scaled - normed * lax.optimization_barrier(jnp.mean(scaled * normed, axis=-1, keepdims=True)))
    return (grad_in, lax.optimization_barrier(jnp.sum(grad_out * normed, axis=0)))

def rotate(values, position):
    half = values.shape[-1] // 2
    inverse = ROPE_BASE ** (-jnp.arange(half, dtype=jnp.float32) / half)
    angle = position.astype(jnp.float32)[:, None] * inverse[None, :]
    cosine = jnp.cos(angle)[:, None, :]
    sine = jnp.sin(angle)[:, None, :]
    first = values[..., :half]
    second = values[..., half:]
    return jnp.concatenate([first * cosine - second * sine, second * cosine + first * sine], axis=-1)

def same_causal(segments):
    count = segments.shape[0]
    order = jnp.arange(count, dtype=jnp.int32)
    return (segments[:, None] == segments[None, :]) & (order[:, None] >= order[None, :])

def attention_core(q_part, kv_part, segments, position):
    count = q_part.shape[0]
    group = QHEADS // KVHEADS
    queries = rotate(q_part.reshape(count, QHEADS, HDIM), position).reshape(count, KVHEADS, group, HDIM)
    keys = rotate(kv_part[:, :KVHEADS * HDIM].reshape(count, KVHEADS, HDIM), position)
    values = kv_part[:, KVHEADS * HDIM:].reshape(count, KVHEADS, HDIM)
    scores = jnp.einsum('tkgd,skd->kgts', queries, keys, precision=lax.Precision.HIGHEST) * HDIM ** (-0.5)
    allowed = same_causal(segments)
    scores = jnp.where(allowed, scores, -1e+30)
    top = lax.optimization_barrier(jnp.max(scores, axis=-1, keepdims=True))
    weights = jnp.exp(scores - top)
    total = lax.optimization_barrier(jnp.sum(weights, axis=-1, keepdims=True))
    mixed = jnp.einsum('kgts,skd->tkgd', weights / total, values, precision=lax.Precision.HIGHEST)
    return mixed.reshape(count, QHEADS * HDIM)

def mamba_core(z_part, x_part, bc_part, dt_part, conv_weight, conv_bias, head_params, segments):
    count = x_part.shape[0]
    mixed_in = jnp.concatenate([x_part, bc_part], axis=1)
    conv_acc = conv_bias[None, :] + conv_weight[0][None, :] * mixed_in
    for shift in range(1, KCONV):
        moved = jnp.concatenate([jnp.zeros((shift, mixed_in.shape[1]), mixed_in.dtype), mixed_in[:-shift]], axis=0)
        linked = jnp.concatenate([jnp.zeros((shift,), dtype=jnp.bool_), segments[shift:] == segments[:-shift]])
        conv_acc = conv_acc + conv_weight[shift][None, :] * jnp.where(linked[:, None], moved, 0.0)
    conved = jax.nn.silu(conv_acc)
    x_conv = conved[:, :DSSM]
    b_conv = conved[:, DSSM:DSSM + NSTATE]
    c_conv = conved[:, DSSM + NSTATE:]
    step_size = jax.nn.softplus(dt_part + head_params[1][None, :])
    log_decay = -step_size * jnp.exp(head_params[0])[None, :]
    running = jnp.cumsum(log_decay, axis=0)
    allowed = same_causal(segments)[:, :, None]
    gap = jnp.where(allowed, running[:, None, :] - running[None, :, :], 0.0)
    inner = jnp.dot(c_conv, b_conv.T, precision=lax.Precision.HIGHEST)
    kernel = jnp.where(allowed, jnp.exp(gap), 0.0) * inner[:, :, None]
    heads_in = x_conv.reshape(count, HEADS, HDIM) * step_size[:, :, None]
    scanned = jnp.einsum('tsh,shp->thp', kernel, heads_in, precision=lax.Precision.HIGHEST)
    scanned = scanned + head_params[2][None, :, None] * x_conv.reshape(count, HEADS, HDIM)
    return scanned.reshape(count, DSSM) * jax.nn.silu(z_part)

def forward_pass(block_input, segments, position, weights, head_params):
    gain_one, w_z, w_x, w_bc, w_dt, conv_weight, conv_bias, w_mout, w_q, w_kv, w_ao, gain_two, w_gate, w_up, w_down = weights
    as_float = block_input.astype(jnp.float32)
    normed_one, rstd_one, normed_in = norm_forward(as_float, gain_one)
    z_part = matmul(normed_in, w_z)
    x_part = matmul(normed_in, w_x)
    bc_part = matmul(normed_in, w_bc)
    dt_part = matmul(normed_in, w_dt)
    q_part = matmul(normed_in, w_q)
    kv_part = matmul(normed_in, w_kv)
    mamba_y = mamba_core(z_part, x_part, bc_part, dt_part, conv_weight.astype(jnp.float32), conv_bias.astype(jnp.float32), head_params, segments).astype(jnp.bfloat16)
    attn_y = attention_core(q_part, kv_part, segments, position).astype(jnp.bfloat16)
    hidden = as_float + matmul(mamba_y, w_mout) + matmul(attn_y, w_ao)
    normed_two, rstd_two, normed_mid = norm_forward(hidden, gain_two)
    gate_pre = matmul(normed_mid, w_gate)
    up_pre = matmul(normed_mid, w_up)
    activated = (jax.nn.silu(gate_pre) * up_pre).astype(jnp.bfloat16)
    block_out = (hidden + matmul(activated, w_down)).astype(jnp.bfloat16)
    saved = (normed_one, rstd_one, normed_in, z_part, x_part, bc_part, dt_part, q_part, kv_part, mamba_y, attn_y, normed_two, rstd_two, normed_mid, gate_pre, up_pre, activated)
    return (block_out, saved)

def backward_ffn(saved, cotangent, weights):
    normed_one, rstd_one, normed_in, z_part, x_part, bc_part, dt_part, q_part, kv_part, mamba_y, attn_y, normed_two, rstd_two, normed_mid, gate_pre, up_pre, activated = saved
    gain_two, w_gate, w_up, w_down = (weights[11], weights[12], weights[13], weights[14])
    grad_act = mat_bt(cotangent, w_down)
    grad_down = mat_at(activated, cotangent)
    sigma = jax.nn.sigmoid(gate_pre)
    grad_up_pre = (grad_act * gate_pre * sigma).astype(jnp.bfloat16)
    grad_gate_pre = (grad_act * up_pre * sigma * (1.0 + gate_pre * (1.0 - sigma))).astype(jnp.bfloat16)
    grad_mid = mat_bt(grad_gate_pre, w_gate) + mat_bt(grad_up_pre, w_up)
    grad_gate = mat_at(normed_mid, grad_gate_pre)
    grad_up = mat_at(normed_mid, grad_up_pre)
    grad_norm, grad_gain_two = norm_backward(grad_mid, normed_two, rstd_two, gain_two)
    grad_hidden = cotangent.astype(jnp.float32) + grad_norm
    return (grad_hidden, (grad_gain_two, grad_gate, grad_up, grad_down))

def backward_mixer(saved, grad_hidden, weights, head_params, segments, position):
    normed_one, rstd_one, normed_in, z_part, x_part, bc_part, dt_part, q_part, kv_part, mamba_y, attn_y, normed_two, rstd_two, normed_mid, gate_pre, up_pre, activated = saved
    gain_one, w_z, w_x, w_bc, w_dt, conv_weight, conv_bias, w_mout, w_q, w_kv, w_ao = weights[:11]
    grad_hidden_b = grad_hidden.astype(jnp.bfloat16)
    grad_attn = mat_bt(grad_hidden_b, w_ao)
    grad_ao = mat_at(attn_y, grad_hidden_b)
    grad_mamba = mat_bt(grad_hidden_b, w_mout)
    grad_mout = mat_at(mamba_y, grad_hidden_b)

    def attend(query_in, keyval_in):
        return attention_core(query_in, keyval_in, segments, position)
    _, attn_pull = jax.vjp(attend, q_part, kv_part)
    grad_q, grad_kv = attn_pull(grad_attn)

    def mixer(gate_in, inner_in, state_in, step_in, conv_in, bias_in, heads_in):
        return mamba_core(gate_in, inner_in, state_in, step_in, conv_in, bias_in, heads_in, segments)
    _, mamba_pull = jax.vjp(mixer, z_part, x_part, bc_part, dt_part, conv_weight.astype(jnp.float32), conv_bias.astype(jnp.float32), head_params)
    grad_z, grad_x, grad_bc, grad_dt, grad_conv, grad_bias, grad_head = mamba_pull(grad_mamba)
    pieces = tuple((piece.astype(jnp.bfloat16) for piece in (grad_z, grad_x, grad_bc, grad_dt, grad_q, grad_kv)))
    matrices = (w_z, w_x, w_bc, w_dt, w_q, w_kv)
    grad_normed = mat_bt(pieces[0], matrices[0])
    for number in range(1, 6):
        grad_normed = grad_normed + mat_bt(pieces[number], matrices[number])
    weight_grads = tuple((mat_at(normed_in, piece) for piece in pieces))
    grad_norm, grad_gain_one = norm_backward(grad_normed, normed_one, rstd_one, gain_one)
    grad_input = (grad_hidden + grad_norm).astype(jnp.bfloat16)
    mixer_grads = (grad_gain_one, weight_grads[0], weight_grads[1], weight_grads[2], weight_grads[3], grad_conv, grad_bias, grad_mout, weight_grads[4], weight_grads[5], grad_ao)
    return (grad_input, mixer_grads, grad_head)

def reference(block_input, segments, cotangent, gain_one, w_z, w_x, w_bc, w_dt, conv_weight, conv_bias, head_params, w_mout, w_q, w_kv, w_ao, gain_two, w_gate, w_up, w_down):
    weights = (gain_one, w_z, w_x, w_bc, w_dt, conv_weight, conv_bias, w_mout, w_q, w_kv, w_ao, gain_two, w_gate, w_up, w_down)
    blocks = TOKENS // ROWS

    def advance(carry, item):
        grads, head_grad = carry
        x_block, seg_block, cot_block, index = item
        position = index * ROWS + jnp.arange(ROWS, dtype=jnp.int32) - seg_block
        block_out, saved = forward_pass(x_block, seg_block, position, weights, head_params)
        grad_hidden, ffn_grads = backward_ffn(saved, cot_block, weights)
        grad_input, mixer_grads, grad_head = backward_mixer(saved, grad_hidden, weights, head_params, seg_block, position)
        ordered = mixer_grads + ffn_grads
        grads = tuple((total + part for total, part in zip(grads, ordered)))
        return ((grads, head_grad + grad_head), (block_out, grad_input))
    start = tuple((jnp.zeros(weight.shape, jnp.float32) for weight in weights))
    items = (block_input.reshape(blocks, ROWS, D), segments.reshape(blocks, ROWS), cotangent.reshape(blocks, ROWS, D), jnp.arange(blocks, dtype=jnp.int32))
    (grads, head_grad), (outputs, grad_inputs) = lax.scan(advance, (start, jnp.zeros((3, HEADS), jnp.float32)), items)
    return (outputs.reshape(TOKENS, D), grad_inputs.reshape(TOKENS, D), grads[0], grads[1], grads[2], grads[3], grads[4], grads[5], grads[6], head_grad, grads[7], grads[8], grads[9], grads[10], grads[11], grads[12], grads[13], grads[14])
```

```python
import functools

import jax
import jax.numpy as jnp
from jax import lax
from jax.experimental import pallas as pl
from jax.experimental.pallas import tpu as pltpu
from jax.sharding import PartitionSpec as P

HEADS = 24
HDIM = 128
NSTATE = 256
KCONV = 4
QHEADS = 12
KVHEADS = 2
DSSM = 3072


EPS = 1e-05
ROPE_BASE = 100000000000.0


def matmul(left, right):
    return jnp.dot(left, right, preferred_element_type=jnp.float32)


def mat_bt(left, right):
    return lax.dot_general(
        left, right, (((1,), (1,)), ((), ())), preferred_element_type=jnp.float32
    )


def mat_at(left, right):
    return lax.dot_general(
        left, right, (((0,), (0,)), ((), ())), preferred_element_type=jnp.float32
    )


def norm_forward(values, gain):
    rstd = lax.rsqrt(jnp.mean(values * values, axis=-1, keepdims=True) + EPS)
    normed = values * rstd
    return (normed, rstd, (normed * gain.astype(jnp.float32)).astype(jnp.bfloat16))


def norm_backward(grad_out, normed, rstd, gain):
    scaled = grad_out * gain.astype(jnp.float32)
    grad_in = rstd * (scaled - normed * jnp.mean(scaled * normed, axis=-1, keepdims=True))
    return (grad_in, jnp.sum(grad_out * normed, axis=0))


def rotate(values, position):
    half = values.shape[-1] // 2
    inverse = ROPE_BASE ** (-jnp.arange(half, dtype=jnp.float32) / half)
    angle = position.astype(jnp.float32)[:, None] * inverse[None, :]
    cosine = jnp.cos(angle)[:, None, :]
    sine = jnp.sin(angle)[:, None, :]
    first = values[..., :half]
    second = values[..., half:]
    return jnp.concatenate(
        [first * cosine - second * sine, second * cosine + first * sine], axis=-1
    )


def same_causal(segments):
    count = segments.shape[0]
    order = jnp.arange(count, dtype=jnp.int32)
    return (segments[:, None] == segments[None, :]) & (order[:, None] >= order[None, :])


def attention_core(q_part, kv_part, segments, position):
    count = q_part.shape[0]
    group = QHEADS // KVHEADS
    queries = rotate(q_part.reshape(count, QHEADS, HDIM), position).reshape(
        count, KVHEADS, group, HDIM
    )
    keys = rotate(kv_part[:, : KVHEADS * HDIM].reshape(count, KVHEADS, HDIM), position)
    values = kv_part[:, KVHEADS * HDIM :].reshape(count, KVHEADS, HDIM)
    scores = jnp.einsum(
        "tkgd,skd->kgts", queries, keys, precision=lax.Precision.HIGHEST
    ) * HDIM ** (-0.5)
    allowed = same_causal(segments)
    scores = jnp.where(allowed, scores, -1e30)
    top = jnp.max(scores, axis=-1, keepdims=True)
    weights = jnp.exp(scores - top)
    total = jnp.sum(weights, axis=-1, keepdims=True)
    mixed = jnp.einsum("kgts,skd->tkgd", weights / total, values, precision=lax.Precision.HIGHEST)
    return mixed.reshape(count, QHEADS * HDIM)


def mamba_core(z_part, x_part, bc_part, dt_part, conv_weight, conv_bias, head_params, segments):
    count = x_part.shape[0]
    mixed_in = jnp.concatenate([x_part, bc_part], axis=1)
    conv_acc = conv_bias[None, :] + conv_weight[0][None, :] * mixed_in
    for shift in range(1, KCONV):
        moved = jnp.concatenate(
            [jnp.zeros((shift, mixed_in.shape[1]), mixed_in.dtype), mixed_in[:-shift]], axis=0
        )
        linked = jnp.concatenate(
            [jnp.zeros((shift,), dtype=jnp.bool_), segments[shift:] == segments[:-shift]]
        )
        conv_acc = conv_acc + conv_weight[shift][None, :] * jnp.where(linked[:, None], moved, 0.0)
    conved = jax.nn.silu(conv_acc)
    x_conv = conved[:, :DSSM]
    b_conv = conved[:, DSSM : DSSM + NSTATE]
    c_conv = conved[:, DSSM + NSTATE :]
    step_size = jax.nn.softplus(dt_part + head_params[1][None, :])
    log_decay = -step_size * jnp.exp(head_params[0])[None, :]
    running = jnp.cumsum(log_decay, axis=0)
    allowed = same_causal(segments)[:, :, None]
    gap = jnp.where(allowed, running[:, None, :] - running[None, :, :], 0.0)
    inner = jnp.dot(c_conv, b_conv.T, precision=lax.Precision.HIGHEST)
    kernel = jnp.where(allowed, jnp.exp(gap), 0.0) * inner[:, :, None]
    heads_in = x_conv.reshape(count, HEADS, HDIM) * step_size[:, :, None]
    scanned = jnp.einsum("tsh,shp->thp", kernel, heads_in, precision=lax.Precision.HIGHEST)
    scanned = scanned + head_params[2][None, :, None] * x_conv.reshape(count, HEADS, HDIM)
    return scanned.reshape(count, DSSM) * jax.nn.silu(z_part)


VMEM_LIMIT = 66000000


class Torus:
    def __init__(self, mesh):
        spots = [device.coords for device in mesh.devices.flat]
        nx, ny, nz = (max(s[a] for s in spots) - min(s[a] for s in spots) + 1 for a in range(3))
        assert nx * ny * nz * 2 == mesh.shape["dp"]
        self.n = mesh.shape["dp"]
        self.nz = nz
        self.plane = 2 * nx * ny
        self.same = nx == ny
        self.n2, self.n3 = ny, nx
        self.far, self.near = 2 * nx, 2

    def order(self):
        return [
            (k, i, j) for k in range(self.nz) for i in range(self.n2) for j in range(self.n3)
        ]


def flip(value, step):
    out, bit = value, 1
    while bit <= step:
        if step & bit:
            out = out + bit - 2 * bit * ((value // bit) % 2)
        bit *= 2
    return out


class Place:
    def __init__(self, torus):
        me = lax.axis_index("dp")
        self.me, self.core = me, me % 2
        self.z = me // torus.plane
        far = (me // torus.far) % torus.n2
        near = (me // torus.near) % torus.n3
        if torus.same:
            self.second = far + self.core * (near - far)
            self.third = near + self.core * (far - near)
            self.step2 = torus.far + self.core * (torus.near - torus.far)
            self.step3 = torus.near + self.core * (torus.far - torus.near)
        else:
            self.second, self.third = far, near
            self.step2, self.step3 = torus.far, torus.near
        self.torus = torus
        self.sibling = me + 1 - 2 * self.core

    def at(self, k, i, j):
        return (
            flip(self.z, k) * self.torus.plane
            + flip(self.second, i) * self.step2
            + flip(self.third, j) * self.step3
            + self.core
        )

    def peers(self):
        t = self.torus
        return (
            [self.at(k, 0, 0) for k in range(1, t.nz)]
            + [self.at(0, i, 0) for i in range(1, t.n2)]
            + [self.at(0, 0, j) for j in range(1, t.n3)]
            + [self.sibling]
        )


def greet(place):
    barrier = pltpu.get_barrier_semaphore()
    peers = place.peers()
    for peer in peers:
        pl.semaphore_signal(
            barrier, inc=1, device_id=(peer,), device_id_type=pl.DeviceIdType.MESH
        )
    pl.semaphore_wait(barrier, len(peers))


def remote(src, dst, send, recv, device):
    return pltpu.make_async_remote_copy(
        src_ref=src,
        dst_ref=dst,
        send_sem=send,
        recv_sem=recv,
        device_id=(device,),
        device_id_type=pl.DeviceIdType.MESH,
    )


def spread(torus, place, ins, outs, send_sem, recv_sem, local_sem):
    count = len(ins)
    started = []

    def push(block, device, own=False):
        for a in range(count):
            source = ins[a] if own else outs[a].at[block]
            copy = remote(
                source,
                outs[a].at[block],
                send_sem.at[a, len(started) // count],
                recv_sem.at[a, block],
                device,
            )
            copy.start()
            started.append(copy)

    def arrive(block):
        for a in range(count):
            remote(
                outs[a].at[block],
                outs[a].at[block],
                send_sem.at[a, 0],
                recv_sem.at[a, block],
                place.sibling,
            ).wait_recv()

    own_copies = [
        pltpu.make_async_copy(ins[a], outs[a].at[place.me], local_sem.at[a])
        for a in range(count)
    ]
    for copy in own_copies:
        copy.start()
    for k, i, j in torus.order():
        block = place.at(k, i, j)
        own = (k, i, j) == (0, 0, 0)
        if not own:
            arrive(block)
        if own:
            for step in range(1, torus.nz):
                push(block, place.at(step, 0, 0), own)
        if i == 0 and j == 0:
            for step in range(1, torus.n2):
                push(block, place.at(0, step, 0), own)
        if j == 0:
            for step in range(1, torus.n3):
                push(block, place.at(0, 0, step), own)
        push(block, place.sibling, own)
    for copy in own_copies:
        copy.wait()
    for k, i, j in torus.order():
        block = other(place, k, i, j)
        arrive(block)
    for copy in started:
        copy.wait_send()


def other(place, k, i, j):
    t = place.torus
    if t.same:
        return (
            flip(place.z, k) * t.plane
            + flip(place.third, i) * place.step3
            + flip(place.second, j) * place.step2
            + (1 - place.core)
        )
    return (
        flip(place.z, k) * t.plane
        + flip(place.second, i) * place.step2
        + flip(place.third, j) * place.step3
        + (1 - place.core)
    )


def sends_of(torus):
    nz, n2, n3 = torus.nz, torus.n2, torus.n3
    return (nz - 1) + nz * (n2 - 1) + nz * n2 * (n3 - 1) + nz * n2 * n3


def gather_kernel(torus, count, *refs):
    ins, outs = refs[:count], refs[count : 2 * count]
    send_sem, recv_sem, local_sem = refs[2 * count :]
    place = Place(torus)
    greet(place)
    spread(torus, place, ins, outs, send_sem, recv_sem, local_sem)


def gather(torus, arrays, name, ident):
    count, n = len(arrays), torus.n
    return pl.pallas_call(
        functools.partial(gather_kernel, torus, count),
        out_shape=[jax.ShapeDtypeStruct((n,) + a.shape, a.dtype) for a in arrays],
        in_specs=[pl.BlockSpec(memory_space=pltpu.VMEM)] * count,
        out_specs=[pl.BlockSpec(memory_space=pl.ANY)] * count,
        scratch_shapes=[
            pltpu.SemaphoreType.DMA((count, sends_of(torus))),
            pltpu.SemaphoreType.DMA((count, n)),
            pltpu.SemaphoreType.DMA((count,)),
        ],
        compiler_params=pltpu.CompilerParams(
            collective_id=ident, has_side_effects=True, vmem_limit_bytes=VMEM_LIMIT
        ),
        name=name,
    )(*arrays)


def scatter_kernel(torus, first, wide, part_ref, out_ref, stage, from_core, from_third, from_second,
                   from_z, load_sem, core_sem, third_sem, second_sem, z_sem, send_sem):
    place = Place(torus)
    greet(place)
    nz, n2, n3 = torus.nz, torus.n2, torus.n3
    order = [(k, i, j) for k in reversed(range(nz)) for i in reversed(range(n2)) for j in reversed(range(n3))]
    columns = pl.ds(first, wide)
    started = []

    def slot_of(k, i, j):
        return (k * n2 + i) * n3 + j

    def send(src, dst, sem, device):
        copy = remote(src, dst, send_sem.at[len(started)], sem, device)
        copy.start()
        started.append(copy)

    def receive(dst, sem):
        remote(dst, dst, send_sem.at[0], sem, place.sibling).wait_recv()

    for k, i, j in order:
        s = slot_of(k, i, j)
        send(part_ref.at[other(place, k, i, j), :, columns], from_core.at[s], core_sem.at[s], place.sibling)

    def load(number):
        k, i, j = order[number]
        return pltpu.make_async_copy(
            part_ref.at[place.at(k, i, j), :, columns], stage.at[number % 2], load_sem.at[number % 2]
        )

    load(0).start()
    for number, (k, i, j) in enumerate(order):
        s = slot_of(k, i, j)
        if number + 1 < len(order):
            load(number + 1).start()
        load(number).wait()
        receive(from_core.at[s], core_sem.at[s])
        add(from_core.at[s], stage.at[number % 2])
        if j:
            t = (k * n2 + i) * (n3 - 1) + j - 1
            send(from_core.at[s], from_third.at[t], third_sem.at[t], place.at(0, 0, j))
    for k in reversed(range(nz)):
        for i in reversed(range(n2)):
            s = slot_of(k, i, 0)
            for j in range(1, n3):
                t = (k * n2 + i) * (n3 - 1) + j - 1
                receive(from_third.at[t], third_sem.at[t])
                add(from_core.at[s], from_third.at[t])
            if i:
                t = k * (n2 - 1) + i - 1
                send(from_core.at[s], from_second.at[t], second_sem.at[t], place.at(0, i, 0))
        s = slot_of(k, 0, 0)
        for i in range(1, n2):
            t = k * (n2 - 1) + i - 1
            receive(from_second.at[t], second_sem.at[t])
            add(from_core.at[s], from_second.at[t])
        if k:
            send(from_core.at[s], from_z.at[k - 1], z_sem.at[k - 1], place.at(k, 0, 0))
    for k in range(1, nz):
        receive(from_z.at[k - 1], z_sem.at[k - 1])
        add(from_core.at[0], from_z.at[k - 1])
    out_ref[...] = from_core[0]
    for copy in started:
        copy.wait_send()


def add(into, term):
    rows = into.shape[0]
    step = 16
    if rows % step:
        into[...] = (into[...].astype(jnp.float32) + term[...].astype(jnp.float32)).astype(into.dtype)
        return

    @pl.loop(0, rows // step)
    def _(index):
        piece = pl.ds(pl.multiple_of(index * step, step), step)
        into[piece, :] = (
            into[piece, :].astype(jnp.float32) + term[piece, :].astype(jnp.float32)
        ).astype(into.dtype)


def scatter(torus, part, name, ident):
    n, rows, width = part.shape
    nz, n2, n3 = torus.nz, torus.n2, torus.n3
    thirds, seconds = nz * n2 * (n3 - 1), nz * (n2 - 1)
    blocks = nz * n2 * n3 + thirds + seconds + nz - 1 + 3
    lanes = -(-width // 128)
    tile = (-(-rows // 16) * 16) * 128 * part.dtype.itemsize
    pieces = 1
    while blocks * tile * -(-lanes // pieces) > VMEM_LIMIT - 6 * 2**20:
        pieces += 1
    wide = -(-lanes // pieces) * 128
    outs = []
    for number, first in enumerate(range(0, width, wide)):
        size = min(wide, width - first)
        block = (rows, size)
        sends = nz * n2 * n3 + thirds + seconds + nz - 1
        outs.append(
            pl.pallas_call(
                functools.partial(scatter_kernel, torus, first, size),
                out_shape=jax.ShapeDtypeStruct(block, part.dtype),
                in_specs=[pl.BlockSpec(memory_space=pl.ANY)],
                out_specs=pl.BlockSpec(memory_space=pltpu.VMEM),
                scratch_shapes=[
                    pltpu.VMEM((2,) + block, part.dtype),
                    pltpu.VMEM((nz * n2 * n3,) + block, part.dtype),
                    pltpu.VMEM((thirds,) + block, part.dtype),
                    pltpu.VMEM((seconds,) + block, part.dtype),
                    pltpu.VMEM((nz - 1,) + block, part.dtype),
                    pltpu.SemaphoreType.DMA((2,)),
                    pltpu.SemaphoreType.DMA((nz * n2 * n3,)),
                    pltpu.SemaphoreType.DMA((thirds,)),
                    pltpu.SemaphoreType.DMA((seconds,)),
                    pltpu.SemaphoreType.DMA((nz - 1,)),
                    pltpu.SemaphoreType.DMA((sends,)),
                ],
                compiler_params=pltpu.CompilerParams(
                    collective_id=ident + number, has_side_effects=True, vmem_limit_bytes=VMEM_LIMIT
                ),
                name=f"{name}_{number}",
            )(part)
        )
    return outs[0] if len(outs) == 1 else jnp.concatenate(outs, axis=1)


def pack_small(parts):
    return jnp.concatenate([part.reshape(-1) for part in parts])


def weave(wide, narrow, ways):
    count = wide.shape[0]
    return jnp.concatenate(
        [wide.reshape(count, ways, -1), narrow.reshape(count, ways, -1)], axis=2
    ).reshape(count, -1)


def per_device(
    torus,
    block_input,
    segments,
    cotangent,
    gain_one,
    w_z,
    w_x,
    w_bc,
    w_dt,
    conv_weight,
    conv_bias,
    head_params,
    w_mout,
    w_q,
    w_kv,
    w_ao,
    gain_two,
    w_gate,
    w_up,
    w_down,
):
    ways = torus.n
    count, width = block_input.shape
    rows = w_z.shape[0]
    position = lax.axis_index("dp") * count + jnp.arange(count, dtype=jnp.int32) - segments
    f32, bf16 = jnp.float32, jnp.bfloat16

    smalls = (gain_one, gain_two, conv_bias, conv_weight.T)
    packed = pack_small(smalls)
    extra = -(-packed.size // rows)
    packed = jnp.pad(packed, (0, extra * rows - packed.size)).reshape(rows, extra)
    projections = (w_z, w_x, w_bc, w_q, w_kv, w_dt)
    edges = [0]
    for w in projections:
        edges.append(edges[-1] + w.shape[1])
    share_in = jnp.concatenate(projections + (packed,), axis=1)
    share_out = jnp.concatenate([w_mout, w_ao], axis=0)
    all_in, all_out = gather(torus, [share_in, share_out], "spread_weights", 1)
    packed_all = all_in[:, :, edges[-1] :].reshape(ways, -1)
    w_in = all_in.reshape(ways * rows, -1)
    w_out = all_out.reshape(-1, width)
    cut = 0
    small_all = []
    for part in smalls:
        piece = packed_all[:, cut : cut + part.size]
        small_all.append(piece.reshape((ways * part.shape[0],) + part.shape[1:]))
        cut += part.size
    gain_one_all, gain_two_all, bias_all, conv_all = small_all
    conv_all = conv_all.T.astype(f32)
    bias_all = bias_all.astype(f32)

    as_float = block_input.astype(f32)
    normed_one, rstd_one, normed_in = norm_forward(as_float, gain_one_all)
    joint = matmul(normed_in, w_in)
    z_part, x_part, bc_part, q_part, kv_part, dt_part = (
        joint[:, edges[k] : edges[k + 1]] for k in range(6)
    )

    def mixer(gate_in, inner_in, state_in, step_in, conv_in, bias_in, heads_in):
        return mamba_core(
            gate_in, inner_in, state_in, step_in, conv_in, bias_in, heads_in, segments
        )

    def attend(query_in, keyval_in):
        return attention_core(query_in, keyval_in, segments, position)

    mamba_out, mamba_pull = jax.vjp(
        mixer, z_part, x_part, bc_part, dt_part, conv_all, bias_all, head_params
    )
    attn_out, attn_pull = jax.vjp(attend, q_part, kv_part)
    mixed = weave(mamba_out.astype(bf16), attn_out.astype(bf16), ways)
    hidden = as_float + matmul(mixed, w_out)
    normed_two, rstd_two, normed_mid = norm_forward(hidden, gain_two_all)

    w_gate_own = lax.all_to_all(w_gate, "dp", split_axis=1, concat_axis=0, tiled=True)
    w_up_own = lax.all_to_all(w_up, "dp", split_axis=1, concat_axis=0, tiled=True)
    cot_all = gather(torus, [cotangent], "spread_cotangent", 2)[0].reshape(-1, width)
    mid_all = gather(torus, [normed_mid], "spread_mid", 3)[0].reshape(-1, width)
    gate_pre = matmul(mid_all, w_gate_own)
    up_pre = matmul(mid_all, w_up_own)
    sigma = jax.nn.sigmoid(gate_pre)
    activated = (gate_pre * sigma * up_pre).astype(bf16)
    grad_act = mat_bt(cot_all, w_down)
    grad_up_pre = (grad_act * gate_pre * sigma).astype(bf16)
    grad_gate_pre = (grad_act * up_pre * sigma * (1.0 + gate_pre * (1.0 - sigma))).astype(bf16)
    mid_share = (mat_bt(grad_gate_pre, w_gate_own) + mat_bt(grad_up_pre, w_up_own)).astype(bf16)
    out_share = matmul(activated, w_down).astype(bf16)
    blocks = (ways, count, width)
    grad_mid = scatter(torus, mid_share.reshape(blocks), "fold_mid", 16).astype(f32)
    out_sum = scatter(torus, out_share.reshape(blocks), "fold_out", 32)
    block_out = (hidden + out_sum.astype(f32)).astype(bf16)
    grad_w_down = mat_at(activated, cot_all)
    grad_w_gate = lax.all_to_all(
        mat_at(mid_all, grad_gate_pre).astype(bf16), "dp", split_axis=0, concat_axis=1, tiled=True
    ).astype(f32)
    grad_w_up = lax.all_to_all(
        mat_at(mid_all, grad_up_pre).astype(bf16), "dp", split_axis=0, concat_axis=1, tiled=True
    ).astype(f32)

    grad_norm, grad_gain_two = norm_backward(grad_mid, normed_two, rstd_two, gain_two_all)
    grad_hidden = cotangent.astype(f32) + grad_norm
    grad_hidden_b = grad_hidden.astype(bf16)
    grad_mixed = mat_bt(grad_hidden_b, w_out).reshape(count, ways, -1)
    grad_mamba = grad_mixed[:, :, :rows].reshape(count, -1)
    grad_attn = grad_mixed[:, :, rows:].reshape(count, -1)
    grad_w_out = scatter(
        torus, mat_at(mixed, grad_hidden_b).astype(bf16).reshape(all_out.shape), "fold_w_out", 48
    ).astype(f32)
    grad_q, grad_kv = attn_pull(grad_attn)
    grad_z, grad_x, grad_bc, grad_dt, grad_conv, grad_bias, grad_head = mamba_pull(grad_mamba)
    pieces = jnp.concatenate(
        [part.astype(bf16) for part in (grad_z, grad_x, grad_bc, grad_q, grad_kv, grad_dt)]
        + [jnp.zeros((count, extra), bf16)],
        axis=1,
    )
    grad_w_in = scatter(
        torus, mat_at(normed_in, pieces).astype(bf16).reshape(all_in.shape), "fold_w_in", 64
    ).astype(f32)
    grad_normed = mat_bt(pieces, w_in)
    grad_w_z, grad_w_x, grad_w_bc, grad_w_q, grad_w_kv, grad_w_dt = (
        grad_w_in[:, edges[k] : edges[k + 1]] for k in range(6)
    )
    grad_norm, grad_gain_one = norm_backward(grad_normed, normed_one, rstd_one, gain_one_all)
    grad_input = (grad_hidden + grad_norm).astype(bf16)

    totals = lax.psum(
        pack_small((grad_gain_one, grad_gain_two, grad_bias, grad_conv.T, grad_head)), "dp"
    )
    own = lax.axis_index("dp")
    cut = 0
    small_grads = []
    for part in smalls:
        piece = totals[cut : cut + ways * part.size].reshape(ways, part.size)
        piece = lax.dynamic_index_in_dim(piece, own, 0, keepdims=False)
        small_grads.append(piece.reshape(part.shape))
        cut += ways * part.size
    head_total = totals[cut:].reshape(head_params.shape)
    return (
        block_out,
        grad_input,
        small_grads[0],
        grad_w_z,
        grad_w_x,
        grad_w_bc,
        grad_w_dt,
        small_grads[3].T,
        small_grads[2],
        head_total,
        grad_w_out[:rows],
        grad_w_q,
        grad_w_kv,
        grad_w_out[rows:],
        small_grads[1],
        grad_w_gate,
        grad_w_up,
        grad_w_down,
    )


def solution(mesh):
    in_specs = (
        P("dp", None),
        P("dp"),
        P("dp", None),
        P("dp"),
        P("dp", None),
        P("dp", None),
        P("dp", None),
        P("dp", None),
        P(None, "dp"),
        P("dp"),
        P(),
        P("dp", None),
        P("dp", None),
        P("dp", None),
        P("dp", None),
        P("dp"),
        P("dp", None),
        P("dp", None),
        P("dp", None),
    )
    out_specs = (
        P("dp", None),
        P("dp", None),
        P("dp"),
        P("dp", None),
        P("dp", None),
        P("dp", None),
        P("dp", None),
        P(None, "dp"),
        P("dp"),
        P(),
        P("dp", None),
        P("dp", None),
        P("dp", None),
        P("dp", None),
        P("dp"),
        P("dp", None),
        P("dp", None),
        P("dp", None),
    )
    return jax.shard_map(
        functools.partial(per_device, Torus(mesh)), mesh=mesh, in_specs=in_specs, out_specs=out_specs, check_vma=False
    )
```

```python
import functools

import jax
import jax.numpy as jnp
from jax import lax
from jax.experimental import pallas as pl
from jax.experimental.layout import Layout, with_layout_constraint
from jax.experimental.pallas import tpu as pltpu
from jax.sharding import PartitionSpec as P


HEADS = 24
HDIM = 128
NSTATE = 256
KCONV = 4
QHEADS = 12
KVHEADS = 2
DSSM = 3072


EPS = 1e-05
ROPE_BASE = 100000000000.0


def matmul(left, right):
    return jnp.dot(left, right, preferred_element_type=jnp.float32)


def mat_bt(left, right):
    return lax.dot_general(
        left, right, (((1,), (1,)), ((), ())), preferred_element_type=jnp.float32
    )


def mat_at(left, right):
    return lax.dot_general(
        left, right, (((0,), (0,)), ((), ())), preferred_element_type=jnp.float32
    )


def norm_forward(values, gain):
    rstd = lax.rsqrt(jnp.mean(values * values, axis=-1, keepdims=True) + EPS)
    normed = values * rstd
    return (normed, rstd, (normed * gain.astype(jnp.float32)).astype(jnp.bfloat16))


def norm_backward(grad_out, normed, rstd, gain):
    scaled = grad_out * gain.astype(jnp.float32)
    grad_in = rstd * (scaled - normed * jnp.mean(scaled * normed, axis=-1, keepdims=True))
    return (grad_in, jnp.sum(grad_out * normed, axis=0))


def rotate(values, position):
    half = values.shape[-1] // 2
    inverse = ROPE_BASE ** (-jnp.arange(half, dtype=jnp.float32) / half)
    angle = position.astype(jnp.float32)[:, None] * inverse[None, :]
    cosine = jnp.cos(angle)[:, None, :]
    sine = jnp.sin(angle)[:, None, :]
    first = values[..., :half]
    second = values[..., half:]
    return jnp.concatenate(
        [first * cosine - second * sine, second * cosine + first * sine], axis=-1
    )


def same_causal(segments):
    count = segments.shape[0]
    order = jnp.arange(count, dtype=jnp.int32)
    return (segments[:, None] == segments[None, :]) & (order[:, None] >= order[None, :])


def attention_core(q_part, kv_part, segments, position):
    count = q_part.shape[0]
    group = QHEADS // KVHEADS
    queries = rotate(q_part.reshape(count, QHEADS, HDIM), position).reshape(
        count, KVHEADS, group, HDIM
    )
    keys = rotate(kv_part[:, : KVHEADS * HDIM].reshape(count, KVHEADS, HDIM), position)
    values = kv_part[:, KVHEADS * HDIM :].reshape(count, KVHEADS, HDIM)
    scores = jnp.einsum(
        "tkgd,skd->kgts", queries, keys, precision=lax.Precision.HIGHEST
    ) * HDIM ** (-0.5)
    allowed = same_causal(segments)
    scores = jnp.where(allowed, scores, -1e30)
    top = jnp.max(scores, axis=-1, keepdims=True)
    weights = jnp.exp(scores - top)
    total = jnp.sum(weights, axis=-1, keepdims=True)
    mixed = jnp.einsum("kgts,skd->tkgd", weights / total, values, precision=lax.Precision.HIGHEST)
    return mixed.reshape(count, QHEADS * HDIM)


def mamba_core(z_part, x_part, bc_part, dt_part, conv_weight, conv_bias, head_params, segments):
    count = x_part.shape[0]
    mixed_in = jnp.concatenate([x_part, bc_part], axis=1)
    conv_acc = conv_bias[None, :] + conv_weight[0][None, :] * mixed_in
    for shift in range(1, KCONV):
        moved = jnp.concatenate(
            [jnp.zeros((shift, mixed_in.shape[1]), mixed_in.dtype), mixed_in[:-shift]], axis=0
        )
        linked = jnp.concatenate(
            [jnp.zeros((shift,), dtype=jnp.bool_), segments[shift:] == segments[:-shift]]
        )
        conv_acc = conv_acc + conv_weight[shift][None, :] * jnp.where(linked[:, None], moved, 0.0)
    conved = jax.nn.silu(conv_acc)
    x_conv = conved[:, :DSSM]
    b_conv = conved[:, DSSM : DSSM + NSTATE]
    c_conv = conved[:, DSSM + NSTATE :]
    step_size = jax.nn.softplus(dt_part + head_params[1][None, :])
    log_decay = -step_size * jnp.exp(head_params[0])[None, :]
    running = jnp.cumsum(log_decay, axis=0)
    allowed = same_causal(segments)[:, :, None]
    gap = jnp.where(allowed, running[:, None, :] - running[None, :, :], 0.0)
    inner = jnp.dot(c_conv, b_conv.T, precision=lax.Precision.HIGHEST)
    kernel = jnp.where(allowed, jnp.exp(gap), 0.0) * inner[:, :, None]
    heads_in = x_conv.reshape(count, HEADS, HDIM) * step_size[:, :, None]
    scanned = jnp.einsum("tsh,shp->thp", kernel, heads_in, precision=lax.Precision.HIGHEST)
    scanned = scanned + head_params[2][None, :, None] * x_conv.reshape(count, HEADS, HDIM)
    return scanned.reshape(count, DSSM) * jax.nn.silu(z_part)


VMEM_LIMIT = 67000000


class Torus:
    def __init__(self, mesh):
        spots = [device.coords for device in mesh.devices.flat]
        nx, ny, nz = (max(s[a] for s in spots) - min(s[a] for s in spots) + 1 for a in range(3))
        assert nx * ny * nz * 2 == mesh.shape["dp"]
        self.n = mesh.shape["dp"]
        self.nz = nz
        self.plane = 2 * nx * ny
        self.same = nx == ny
        self.n2, self.n3 = ny, nx
        self.far, self.near = 2 * nx, 2

    def order(self):
        return [
            (k, i, j) for k in range(self.nz) for i in range(self.n2) for j in range(self.n3)
        ]


def flip(value, step):
    out, bit = value, 1
    while bit <= step:
        if step & bit:
            out = out + bit - 2 * bit * ((value // bit) % 2)
        bit *= 2
    return out


class Place:
    def __init__(self, torus):
        me = lax.axis_index("dp")
        self.me, self.core = me, me % 2
        self.z = me // torus.plane
        far = (me // torus.far) % torus.n2
        near = (me // torus.near) % torus.n3
        if torus.same:
            self.second = far + self.core * (near - far)
            self.third = near + self.core * (far - near)
            self.step2 = torus.far + self.core * (torus.near - torus.far)
            self.step3 = torus.near + self.core * (torus.far - torus.near)
        else:
            self.second, self.third = far, near
            self.step2, self.step3 = torus.far, torus.near
        self.torus = torus
        self.sibling = me + 1 - 2 * self.core

    def at(self, k, i, j):
        return (
            flip(self.z, k) * self.torus.plane
            + flip(self.second, i) * self.step2
            + flip(self.third, j) * self.step3
            + self.core
        )

    def peers(self):
        t = self.torus
        return (
            [self.at(k, 0, 0) for k in range(1, t.nz)]
            + [self.at(0, i, 0) for i in range(1, t.n2)]
            + [self.at(0, 0, j) for j in range(1, t.n3)]
            + [self.sibling]
        )


def greet(place):
    barrier = pltpu.get_barrier_semaphore()
    peers = place.peers()
    for peer in peers:
        pl.semaphore_signal(
            barrier, inc=1, device_id=(peer,), device_id_type=pl.DeviceIdType.MESH
        )
    pl.semaphore_wait(barrier, len(peers))


def remote(src, dst, send, recv, device):
    return pltpu.make_async_remote_copy(
        src_ref=src,
        dst_ref=dst,
        send_sem=send,
        recv_sem=recv,
        device_id=(device,),
        device_id_type=pl.DeviceIdType.MESH,
    )


def spread(torus, place, ins, outs, send_sem, recv_sem, local_sem):
    count = len(ins)
    started = []

    def push(block, device, own=False):
        for a in range(count):
            source = ins[a] if own else outs[a].at[block]
            copy = remote(
                source,
                outs[a].at[block],
                send_sem.at[a, len(started) // count],
                recv_sem.at[a, block],
                device,
            )
            copy.start()
            started.append(copy)

    def arrive(block):
        for a in range(count):
            remote(
                outs[a].at[block],
                outs[a].at[block],
                send_sem.at[a, 0],
                recv_sem.at[a, block],
                place.sibling,
            ).wait_recv()

    own_copies = [
        pltpu.make_async_copy(ins[a], outs[a].at[place.me], local_sem.at[a])
        for a in range(count)
    ]
    for copy in own_copies:
        copy.start()
    late = []
    for k in range(torus.nz):
        for i in range(torus.n2):
            block, own = place.at(k, i, 0), (k, i) == (0, 0)
            if own:
                for step in range(1, torus.nz):
                    push(block, place.at(step, 0, 0), own)
            else:
                arrive(block)
            if i == 0:
                for step in range(1, torus.n2):
                    push(block, place.at(0, step, 0), own)
            for step in range(1, torus.n3):
                push(block, place.at(0, 0, step), own)
            push(block, place.sibling, own)
            for block in late:
                arrive(block)
                push(block, place.sibling)
            late = [place.at(k, i, j) for j in range(1, torus.n3)]
    for block in late:
        arrive(block)
        push(block, place.sibling)
    for copy in own_copies:
        copy.wait()
    for k, i, j in torus.order():
        block = other(place, k, i, j)
        arrive(block)
    for copy in started:
        copy.wait_send()


def other(place, k, i, j):
    t = place.torus
    if t.same:
        return (
            flip(place.z, k) * t.plane
            + flip(place.third, i) * place.step3
            + flip(place.second, j) * place.step2
            + (1 - place.core)
        )
    return (
        flip(place.z, k) * t.plane
        + flip(place.second, i) * place.step2
        + flip(place.third, j) * place.step3
        + (1 - place.core)
    )


def sends_of(torus):
    nz, n2, n3 = torus.nz, torus.n2, torus.n3
    return (nz - 1) + nz * (n2 - 1) + nz * n2 * (n3 - 1) + nz * n2 * n3


def gather_kernel(torus, count, *refs):
    ins, outs = refs[:count], refs[count : 2 * count]
    send_sem, recv_sem, local_sem = refs[2 * count :]
    place = Place(torus)
    greet(place)
    spread(torus, place, ins, outs, send_sem, recv_sem, local_sem)


def gather(torus, arrays, ident):
    count, n = len(arrays), torus.n
    return pl.pallas_call(
        functools.partial(gather_kernel, torus, count),
        out_shape=[jax.ShapeDtypeStruct((n,) + a.shape, a.dtype) for a in arrays],
        in_specs=[pl.BlockSpec(memory_space=pltpu.VMEM)] * count,
        out_specs=[pl.BlockSpec(memory_space=pl.ANY)] * count,
        scratch_shapes=[
            pltpu.SemaphoreType.DMA((count, sends_of(torus))),
            pltpu.SemaphoreType.DMA((count, n)),
            pltpu.SemaphoreType.DMA((count,)),
        ],
        compiler_params=pltpu.CompilerParams(
            collective_id=ident, has_side_effects=True, vmem_limit_bytes=VMEM_LIMIT
        ),
    )(*arrays)


def add(into, term):
    rows = into.shape[0]
    step = 16
    if rows % step:
        into[...] = (into[...].astype(jnp.float32) + term[...].astype(jnp.float32)).astype(into.dtype)
        return

    @pl.loop(0, rows // step)
    def _(index):
        piece = pl.ds(pl.multiple_of(index * step, step), step)
        into[piece, :] = (
            into[piece, :].astype(jnp.float32) + term[piece, :].astype(jnp.float32)
        ).astype(into.dtype)


def scatter_kernel(
    torus,
    first,
    wide,
    part_ref,
    out_ref,
    stage,
    from_core,
    from_third,
    from_second,
    from_z,
    load_sem,
    core_sem,
    third_sem,
    second_sem,
    z_sem,
    send_sem,
):
    place = Place(torus)
    greet(place)
    nz, n2, n3 = torus.nz, torus.n2, torus.n3
    order = [(k, i, j) for k in reversed(range(nz)) for i in reversed(range(n2)) for j in reversed(range(n3))]
    columns = pl.ds(first, wide)
    started = []

    def slot_of(k, i, j):
        return (k * n2 + i) * n3 + j

    def send(src, dst, sem, device):
        copy = remote(src, dst, send_sem.at[len(started)], sem, device)
        copy.start()
        started.append(copy)

    def receive(dst, sem):
        remote(dst, dst, send_sem.at[0], sem, place.sibling).wait_recv()

    for k, i, j in order:
        s = slot_of(k, i, j)
        send(part_ref.at[other(place, k, i, j), :, columns], from_core.at[s], core_sem.at[s], place.sibling)

    def load(number):
        k, i, j = order[number]
        return pltpu.make_async_copy(
            part_ref.at[place.at(k, i, j), :, columns], stage.at[number % 2], load_sem.at[number % 2]
        )

    load(0).start()
    for number, (k, i, j) in enumerate(order):
        s = slot_of(k, i, j)
        if number + 1 < len(order):
            load(number + 1).start()
        load(number).wait()
        receive(from_core.at[s], core_sem.at[s])
        add(from_core.at[s], stage.at[number % 2])
        if j:
            t = (k * n2 + i) * (n3 - 1) + j - 1
            send(from_core.at[s], from_third.at[t], third_sem.at[t], place.at(0, 0, j))
    for k in reversed(range(nz)):
        for i in reversed(range(n2)):
            s = slot_of(k, i, 0)
            for j in range(1, n3):
                t = (k * n2 + i) * (n3 - 1) + j - 1
                receive(from_third.at[t], third_sem.at[t])
                add(from_core.at[s], from_third.at[t])
            if i:
                t = k * (n2 - 1) + i - 1
                send(from_core.at[s], from_second.at[t], second_sem.at[t], place.at(0, i, 0))
        s = slot_of(k, 0, 0)
        for i in range(1, n2):
            t = k * (n2 - 1) + i - 1
            receive(from_second.at[t], second_sem.at[t])
            add(from_core.at[s], from_second.at[t])
        if k:
            send(from_core.at[s], from_z.at[k - 1], z_sem.at[k - 1], place.at(k, 0, 0))
    out_ref[...] = from_core[0].astype(out_ref.dtype)
    for k in range(1, nz):
        receive(from_z.at[k - 1], z_sem.at[k - 1])
        add(out_ref, from_z.at[k - 1])
    for copy in started:
        copy.wait_send()


def scatter(torus, part, ident):
    _, rows, width = part.shape
    nz, n2, n3 = torus.nz, torus.n2, torus.n3
    thirds, seconds = nz * n2 * (n3 - 1), nz * (n2 - 1)
    blocks = nz * n2 * n3 + thirds + seconds + nz - 1 + 4
    lanes = -(-width // 128)
    tile = (-(-rows // 16) * 16) * 128 * part.dtype.itemsize
    pieces = 1
    while blocks * tile * -(-lanes // pieces) > VMEM_LIMIT - 2**20:
        pieces += 1
    wide = -(-lanes // pieces) * 128
    outs = []
    for number, first in enumerate(range(0, width, wide)):
        size = min(wide, width - first)
        block = (rows, size)
        sends = nz * n2 * n3 + thirds + seconds + nz - 1
        outs.append(
            pl.pallas_call(
                functools.partial(scatter_kernel, torus, first, size),
                out_shape=jax.ShapeDtypeStruct(block, jnp.float32),
                in_specs=[pl.BlockSpec(memory_space=pl.ANY)],
                out_specs=pl.BlockSpec(memory_space=pltpu.VMEM),
                scratch_shapes=[
                    pltpu.VMEM((2,) + block, part.dtype),
                    pltpu.VMEM((nz * n2 * n3,) + block, part.dtype),
                    pltpu.VMEM((thirds,) + block, part.dtype),
                    pltpu.VMEM((seconds,) + block, part.dtype),
                    pltpu.VMEM((nz - 1,) + block, part.dtype),
                    pltpu.SemaphoreType.DMA((2,)),
                    pltpu.SemaphoreType.DMA((nz * n2 * n3,)),
                    pltpu.SemaphoreType.DMA((thirds,)),
                    pltpu.SemaphoreType.DMA((seconds,)),
                    pltpu.SemaphoreType.DMA((nz - 1,)),
                    pltpu.SemaphoreType.DMA((sends,)),
                ],
                compiler_params=pltpu.CompilerParams(
                    collective_id=ident + number, has_side_effects=True, vmem_limit_bytes=VMEM_LIMIT
                ),
            )(part)
        )
    return outs[0] if len(outs) == 1 else jnp.concatenate(outs, axis=1)


def ffn_kernel(units, mid_ref, cot_ref, pair_ref, down_ref, act_ref, grad_ref, mid_share_ref, out_share_ref):
    f32, bf16 = jnp.float32, jnp.bfloat16
    pre = jnp.dot(mid_ref[...], pair_ref[...], preferred_element_type=f32)
    grad_act = mat_bt(cot_ref[...], down_ref[...])
    gate, up = pre[:, :units], pre[:, units : 2 * units]
    sigma = jax.nn.sigmoid(gate)
    act = (gate * sigma * up).astype(bf16)
    act_ref[...] = act
    grad_ref[:, :units] = (grad_act * up * sigma * (1.0 + gate * (1.0 - sigma))).astype(bf16)
    grad_ref[:, units:] = (grad_act * gate * sigma).astype(bf16)
    mid_share_ref[...] = mat_bt(grad_ref[...], pair_ref[...]).astype(bf16)
    out_share_ref[...] = jnp.dot(act, down_ref[...], preferred_element_type=f32).astype(bf16)


def feed_forward(mid, cot, pair, down, step):
    tokens, width = mid.shape
    units = down.shape[0]
    bf16 = jnp.bfloat16
    whole = lambda i: (0, 0)
    part = lambda i: (i, 0)
    return pl.pallas_call(
        functools.partial(ffn_kernel, units),
        grid=(tokens // step,),
        out_shape=[
            jax.ShapeDtypeStruct((tokens, units), bf16),
            jax.ShapeDtypeStruct((tokens, 2 * units), bf16),
            jax.ShapeDtypeStruct((tokens, width), bf16),
            jax.ShapeDtypeStruct((tokens, width), bf16),
        ],
        in_specs=[
            pl.BlockSpec((step, width), part),
            pl.BlockSpec((step, width), part),
            pl.BlockSpec(pair.shape, whole, pipeline_mode=pl.Buffered(1)),
            pl.BlockSpec(down.shape, whole, pipeline_mode=pl.Buffered(1)),
        ],
        out_specs=[
            pl.BlockSpec((step, units), part),
            pl.BlockSpec((step, 2 * units), part),
            pl.BlockSpec((step, width), part),
            pl.BlockSpec((step, width), part),
        ],
        compiler_params=pltpu.CompilerParams(vmem_limit_bytes=VMEM_LIMIT),
        cost_estimate=pl.CostEstimate(
            flops=12 * tokens * width * units,
            bytes_accessed=8 * tokens * width,
            transcendentals=tokens * units,
        ),
        name="feed_forward",
    )(mid, cot, pair, down)


def pack_small(parts):
    return jnp.concatenate([part.reshape(-1) for part in parts])


def weave(wide, narrow, ways):
    count = wide.shape[0]
    return jnp.concatenate(
        [wide.reshape(count, ways, -1), narrow.reshape(count, ways, -1)], axis=2
    ).reshape(count, -1)


def per_device(
    torus,
    block_input,
    segments,
    cotangent,
    gain_one,
    w_z,
    w_x,
    w_bc,
    w_dt,
    conv_weight,
    conv_bias,
    head_params,
    w_mout,
    w_q,
    w_kv,
    w_ao,
    gain_two,
    w_gate,
    w_up,
    w_down,
):
    ways = torus.n
    count, width = block_input.shape
    rows = w_z.shape[0]
    position = lax.axis_index("dp") * count + jnp.arange(count, dtype=jnp.int32) - segments
    f32, bf16 = jnp.float32, jnp.bfloat16

    smalls = (gain_one, gain_two, conv_bias, conv_weight.T)
    packed = pack_small(smalls)
    extra = -(-packed.size // rows)
    packed = jnp.pad(packed, (0, extra * rows - packed.size)).reshape(rows, extra)
    projections = (w_z, w_x, w_bc, w_q, w_kv, w_dt)
    edges = [0]
    for w in projections:
        edges.append(edges[-1] + w.shape[1])
    share_in = jnp.concatenate(projections + (packed,), axis=1)
    share_out = jnp.concatenate([w_mout, w_ao], axis=0)
    all_in, all_out = gather(torus, [share_in, share_out], 1)
    packed_all = all_in[:, :, edges[-1] :].reshape(ways, -1)
    w_in = all_in.reshape(ways * rows, -1)
    w_out = all_out.reshape(-1, width)
    cut = 0
    small_all = []
    for part in smalls:
        piece = packed_all[:, cut : cut + part.size]
        small_all.append(piece.reshape((ways * part.shape[0],) + part.shape[1:]))
        cut += part.size
    gain_one_all, gain_two_all, bias_all, conv_all = small_all
    conv_all = conv_all.T.astype(f32)
    bias_all = bias_all.astype(f32)

    as_float = block_input.astype(f32)
    normed_one, rstd_one, normed_in = norm_forward(as_float, gain_one_all)
    joint = matmul(normed_in, w_in)
    z_part, x_part, bc_part, q_part, kv_part, dt_part = (
        joint[:, edges[k] : edges[k + 1]] for k in range(6)
    )

    def mixer(gate_in, inner_in, state_in, step_in, conv_in, bias_in, heads_in):
        return mamba_core(
            gate_in, inner_in, state_in, step_in, conv_in, bias_in, heads_in, segments
        )

    def attend(query_in, keyval_in):
        return attention_core(query_in, keyval_in, segments, position)

    mamba_out, mamba_pull = jax.vjp(
        mixer, z_part, x_part, bc_part, dt_part, conv_all, bias_all, head_params
    )
    attn_out, attn_pull = jax.vjp(attend, q_part, kv_part)
    mixed = weave(mamba_out.astype(bf16), attn_out.astype(bf16), ways)
    hidden = as_float + matmul(mixed, w_out)
    normed_two, rstd_two, normed_mid = norm_forward(hidden, gain_two_all)

    hidden_units = w_gate.shape[1] // ways
    w_pair = jnp.concatenate(
        [w.reshape(rows, ways, hidden_units) for w in (w_gate, w_up)], axis=2
    ).reshape(rows, -1)
    w_pair = lax.all_to_all(w_pair, "dp", split_axis=1, concat_axis=0, tiled=True)
    cot_own, packed_all = lax.optimization_barrier((cotangent, packed_all))
    cot_all = lax.all_gather(cot_own, "dp", axis=0, tiled=True)
    mid_all = gather(torus, [normed_mid], 3)[0].reshape(-1, width)
    activated, grad_pre, mid_share, out_share = feed_forward(mid_all, cot_all, w_pair, w_down, 2 * count)
    out_sum = lax.psum_scatter(out_share, "dp", scatter_dimension=0, tiled=True)
    grad_mid = scatter(torus, mid_share.reshape(ways, count, width), 16)
    grad_w_down = mat_at(activated, cot_all)
    grad_pair = mat_at(mid_all, grad_pre).astype(bf16)
    grad_mid, grad_pair, grad_w_down = lax.optimization_barrier((grad_mid, grad_pair, grad_w_down))
    grad_pair = lax.all_to_all(grad_pair, "dp", split_axis=0, concat_axis=1, tiled=True)
    grad_pair = grad_pair.reshape(rows, ways, 2, hidden_units)
    grad_w_gate = grad_pair[:, :, 0].reshape(rows, -1).astype(f32)
    grad_w_up = grad_pair[:, :, 1].reshape(rows, -1).astype(f32)

    grad_norm, grad_gain_two = norm_backward(grad_mid, normed_two, rstd_two, gain_two_all)
    grad_hidden = cotangent.astype(f32) + grad_norm
    grad_hidden_b = grad_hidden.astype(bf16)
    grad_mixed = mat_bt(grad_hidden_b, w_out)
    grad_mixed = grad_mixed.reshape(count, ways, -1)
    grad_mamba = grad_mixed[:, :, :rows].reshape(count, -1)
    grad_attn = grad_mixed[:, :, rows:].reshape(count, -1)
    grad_w_out = mat_at(mixed, grad_hidden_b).astype(bf16).reshape(all_out.shape)
    grad_w_out = scatter(torus, grad_w_out, 48)
    grad_q, grad_kv = attn_pull(grad_attn)
    grad_z, grad_x, grad_bc, grad_dt, grad_conv, grad_bias, grad_head = mamba_pull(grad_mamba)
    pieces = jnp.concatenate(
        [part.astype(bf16) for part in (grad_z, grad_x, grad_bc, grad_q, grad_kv, grad_dt)]
        + [jnp.zeros((count, extra), bf16)],
        axis=1,
    )
    pieces = with_layout_constraint(pieces, Layout((1, 0)))
    upright = with_layout_constraint(lax.optimization_barrier(pieces), Layout((0, 1)))
    grad_w_in = with_layout_constraint(mat_at(normed_in, upright).astype(bf16), Layout((0, 1)))
    grad_w_in = scatter(torus, grad_w_in.reshape(all_in.shape), 64)
    grad_normed = mat_bt(pieces, w_in)
    grad_w_z, grad_w_x, grad_w_bc, grad_w_q, grad_w_kv, grad_w_dt = (
        grad_w_in[:, edges[k] : edges[k + 1]] for k in range(6)
    )
    grad_norm, grad_gain_one = norm_backward(grad_normed, normed_one, rstd_one, gain_one_all)
    grad_input = (grad_hidden + grad_norm).astype(bf16)
    late, grad_input = lax.optimization_barrier((hidden, grad_input))
    block_out = (late + out_sum.astype(f32)).astype(bf16)

    totals = lax.psum(
        pack_small((grad_gain_one, grad_gain_two, grad_bias, grad_conv.T, grad_head)), "dp"
    )
    own = lax.axis_index("dp")
    cut = 0
    small_grads = []
    for part in smalls:
        piece = totals[cut : cut + ways * part.size].reshape(ways, part.size)
        piece = lax.dynamic_index_in_dim(piece, own, 0, keepdims=False)
        small_grads.append(piece.reshape(part.shape))
        cut += ways * part.size
    head_total = totals[cut:].reshape(head_params.shape)
    return (
        block_out,
        grad_input,
        small_grads[0],
        grad_w_z,
        grad_w_x,
        grad_w_bc,
        grad_w_dt,
        small_grads[3].T,
        small_grads[2],
        head_total,
        grad_w_out[:rows],
        grad_w_q,
        grad_w_kv,
        grad_w_out[rows:],
        small_grads[1],
        grad_w_gate,
        grad_w_up,
        grad_w_down,
    )


def solution(mesh):
    in_specs = (
        P("dp", None),
        P("dp"),
        P("dp", None),
        P("dp"),
        P("dp", None),
        P("dp", None),
        P("dp", None),
        P("dp", None),
        P(None, "dp"),
        P("dp"),
        P(),
        P("dp", None),
        P("dp", None),
        P("dp", None),
        P("dp", None),
        P("dp"),
        P("dp", None),
        P("dp", None),
        P("dp", None),
    )
    out_specs = (
        P("dp", None),
        P("dp", None),
        P("dp"),
        P("dp", None),
        P("dp", None),
        P("dp", None),
        P("dp", None),
        P(None, "dp"),
        P("dp"),
        P(),
        P("dp", None),
        P("dp", None),
        P("dp", None),
        P("dp", None),
        P("dp"),
        P("dp", None),
        P("dp", None),
        P("dp", None),
    )
    return jax.shard_map(
        functools.partial(per_device, Torus(mesh)), mesh=mesh, in_specs=in_specs, out_specs=out_specs, check_vma=False
    )
```
